128 devices in a mesh: dev: 128 (over x, z, y, core).
Axes of the slice: x: 4, y: 4, z: 4, core: 2. Of those that a mesh axis runs over, the one named last changes fastest.
Arguments:
- pixels: float32 [4, 2048, 8192], P(None, 'dev'), may hold values from -10 to 10
- valid_flags: int32 [4, 2048, 8192], P(None, 'dev'), may hold values 0 or 1
Outputs:
- tile_halves: float32 [128, 256, 2048], P('dev')
- header: float32 [5, 4], replicated
The draws below stay inside these ranges and needn't reach their ends.
All inputs are finite; a program needn't handle non-finite values. No bound on the sum of `valid_flags` on one device may be relied on, other than what follows from the above.
Results may differ from the reference program's by a relative error of at most 0.00002.
Values sent between devices are 32-bit elements; how exact they have to be, the bound alone decides.
No kernel may reach another device: no remote copies, remote signals or barrier semaphores. Data moves between devices by JAX's collectives and lax.ppermute only.
A program may use at most 128 MiB of HBM per device.

```python
import jax
import jax.numpy as jnp
from jax import lax

BANDS = 4
TILE = 512
STRIP = 16
GROUP = 16
COLS = 8192
ROWS = 2048
HALF = 256
N_DEV = 128


def draw_pixels(key, part):
    first_key, second_key, third_key = jax.random.split(jax.random.fold_in(key, 11), 3)
    strip_count = ROWS // STRIP
    offsets = jax.random.uniform(first_key, (BANDS, strip_count, 1, 1), jnp.float32, -2.0, 2.0)
    widths = jnp.exp(jax.random.uniform(second_key, (BANDS, strip_count, 1, 1), jnp.float32, jnp.log(0.5), jnp.log(2.0)))
    noise = jnp.clip(jax.random.normal(third_key, (BANDS, strip_count, STRIP, COLS), jnp.float32), -4.0, 4.0)
    values = offsets + widths * noise
    return values.reshape(BANDS, ROWS, COLS).astype(jnp.float32)


def set_ends(result, own_key, low, high):
    longest = result.shape.index(max(result.shape))
    spots = []
    for shift in (0, 1):
        where = [jax.random.randint(jax.random.fold_in(own_key, axis), (), 0, length) for axis, length in enumerate(result.shape)]
        where[longest] = (where[longest] + shift) % result.shape[longest]
        spots.append(tuple(where))
    return result.at[spots[0]].set(low).at[spots[1]].set(high)


def setup_inputs(seed: int = 0) -> dict:
    streams_of = jax.random.split(jax.random.key(seed), 3)
    pixels = draw_pixels(jax.random.fold_in(streams_of[2], 71), 0)
    valid_flags = set_ends((jax.random.randint(streams_of[1], (BANDS, ROWS, COLS), 0, 4) < 3).astype(jnp.int32), jax.random.fold_in(streams_of[1], 1), 0, 1)
    return dict(pixels=pixels, valid_flags=valid_flags)


largest_value = 3e+38

def reference(pixels, valid_flags):
    usable = valid_flags == 1
    filled = jnp.where(usable, pixels, jnp.float32(0.0))
    blocks = filled.reshape(BANDS, ROWS // HALF, HALF, GROUP, TILE)
    tile_halves = jnp.transpose(blocks, (1, 3, 2, 4, 0)).reshape(N_DEV, HALF, TILE * BANDS)
    lowest = lax.optimization_barrier(jnp.min(jnp.where(usable, pixels, jnp.float32(largest_value)), axis=(1, 2)))
    highest = lax.optimization_barrier(jnp.max(jnp.where(usable, pixels, jnp.float32(-largest_value)), axis=(1, 2)))
    valid_count = lax.optimization_barrier(jnp.sum(usable.astype(jnp.float32), axis=(1, 2)))
    band_sum = lax.optimization_barrier(jnp.sum(filled, axis=(1, 2)))
    band_squares = lax.optimization_barrier(jnp.sum(filled * filled, axis=(1, 2)))
    divisor = jnp.maximum(valid_count, 1.0)
    average = band_sum / divisor
    variance = band_squares / divisor - average * average
    header = jnp.stack([lowest, highest, valid_count / (ROWS * COLS), average, jnp.sqrt(jnp.maximum(variance, 0.25))])
    return (tile_halves, header)
```

```python
import functools

import jax
import jax.numpy as jnp
from jax import lax
from jax.experimental import pallas as pl
from jax.experimental.pallas import tpu as pltpu
from jax.sharding import Mesh
from jax.sharding import PartitionSpec as P


BANDS = 4
TILE = 512
STRIP = 16
WIDE = TILE * BANDS
CELLS = 16777216
BIG = 3e38
ALL = ("x", "zh", "z", "y", "c")
GROUP = ("z", "y", "c")
f32 = jnp.float32


Z, Y1, Y2, Y3, ZY1, ZY2, ZY3 = 8, 2, 4, 6, 10, 12, 14
PAIRS = [(ZY1, Y3), (Y1, ZY3), (ZY3, Y1), (Y3, ZY1), (Z, Y2), (Y2, Z), (ZY2, ZY2)]
SLOTS = []
for _a, _b in PAIRS:
    SLOTS += [(_a, _b), (_a | 1, _b | 1)]
SLOTS += [(1, 1), (0, 0)]
CHUNKS = [range(0, 4), range(4, 8), range(8, 12), range(12, 16)]


def position():
    z, y, c = (lax.axis_index(a) for a in GROUP)
    return z * 8 + y * 2 + c, c


def interleave(a, lane, pick):
    low = lane < 64
    even = (lane & 32) == 0
    u0 = jnp.where(low, a[0], pltpu.roll(a[2], 64, 1))
    u2 = jnp.where(low, pltpu.roll(a[0], 64, 1), a[2])
    u1 = jnp.where(low, a[1], pltpu.roll(a[3], 64, 1))
    u3 = jnp.where(low, pltpu.roll(a[1], 64, 1), a[3])
    v = [
        jnp.where(even, u0, pltpu.roll(u1, 32, 1)),
        jnp.where(even, pltpu.roll(u0, 96, 1), u1),
        jnp.where(even, u2, pltpu.roll(u3, 32, 1)),
        jnp.where(even, pltpu.roll(u2, 96, 1), u3),
    ]
    return [jnp.take_along_axis(t, pick, axis=1, mode="promise_in_bounds") for t in v]


def pieces_kernel(slots, first, last, *refs):
    refs = list(refs)
    px, fl = refs[:2]
    del refs[:2]
    acc_in = None if first else refs.pop(0)
    n = len(slots)
    outs = refs[:n]
    acc_out, pbuf, fbuf, sems = refs[n:]
    pos, core = position()
    copies = []
    for i, (k0, k1) in enumerate(slots):
        tile = pos ^ jnp.where(core == 0, k0, k1)
        cols = pl.ds(pl.multiple_of(tile * TILE, TILE), TILE)
        pair = (
            pltpu.make_async_copy(px.at[:, :, cols], pbuf.at[i], sems.at[0, i]),
            pltpu.make_async_copy(fl.at[:, :, cols], fbuf.at[i], sems.at[1, i]),
        )
        for copy in pair:
            copy.start()
        copies.append(pair)
    lane = lax.broadcasted_iota(jnp.int32, (8, 128), 1)
    pick = 32 * (lane & 3) + (lane >> 2)
    if first:
        acc = [jnp.full((8, 128), -BIG, f32)] * 8 + [jnp.zeros((8, 128), f32)] * 12
    else:
        acc = [acc_in[s] for s in range(20)]
    for i in range(n):
        for copy in copies[i]:
            copy.wait()
        for r in (0, 8):
            for s in range(TILE // 128):
                part = []
                for b in range(BANDS):
                    v = pbuf[i, b, r : r + 8, s * 128 : s * 128 + 128]
                    use = fbuf[i, b, r : r + 8, s * 128 : s * 128 + 128] == 1
                    m = jnp.where(use, v, 0.0)
                    acc[b] = jnp.maximum(acc[b], jnp.where(use, -v, -BIG))
                    acc[4 + b] = jnp.maximum(acc[4 + b], jnp.where(use, v, -BIG))
                    acc[8 + b] += jnp.where(use, 1.0, 0.0)
                    acc[12 + b] += m
                    acc[16 + b] += m * m
                    part.append(m)
                for j, o in enumerate(interleave(part, lane, pick)):
                    outs[i][r : r + 8, s * 512 + j * 128 : s * 512 + j * 128 + 128] = o
    if last:
        for s in range(20):
            reduce = jnp.max if s < 8 else jnp.sum
            acc_out[s : s + 1, :] = reduce(acc[s], axis=0, keepdims=True)
        acc_out[20:24, :] = jnp.zeros((4, 128), f32)
    else:
        for s in range(20):
            acc_out[s] = acc[s]


def pieces(slots, pixels, flags, acc, last):
    n = len(slots)
    first = acc is None
    any_ = pl.BlockSpec(memory_space=pltpu.HBM)
    vmem = pl.BlockSpec(memory_space=pltpu.VMEM)
    stat = jax.ShapeDtypeStruct((24, 128) if last else (20, 8, 128), f32)
    out = pl.pallas_call(
        functools.partial(pieces_kernel, slots, first, last),
        out_shape=[jax.ShapeDtypeStruct((STRIP, WIDE), f32)] * n + [stat],
        in_specs=[any_, any_] + ([] if first else [vmem]),
        out_specs=[vmem] * (n + 1),
        scratch_shapes=[
            pltpu.VMEM((n, BANDS, STRIP, TILE), f32),
            pltpu.VMEM((n, BANDS, STRIP, TILE), jnp.int32),
            pltpu.SemaphoreType.DMA((2, n)),
        ],
        compiler_params=pltpu.CompilerParams(vmem_limit_bytes=12 << 20),
        cost_estimate=pl.CostEstimate(flops=4_000_000, bytes_accessed=n * 393216, transcendentals=0),
    )(pixels, flags, *([] if first else [acc]))
    return out[:n], out[n]


def merged(a, b):
    row = lax.broadcasted_iota(jnp.int32, (24, 128), 0)
    return jnp.where(row < 8, jnp.maximum(a, b), a + b)


def assemble_kernel(slots, header, *refs):
    n = len(slots)
    refs = list(refs)
    if header:
        stats = refs[:8]
        del refs[:9]
    ins = refs[:n]
    out = refs[n]
    sems = refs[-1]
    pos, core = position()
    copies = []
    for i, (k0, k1) in enumerate(slots):
        key = jnp.where((core ^ (k0 & 1)) == 0, k0, k1)
        rows = pl.ds(pl.multiple_of((pos ^ key) * STRIP, STRIP), STRIP)
        copies.append(pltpu.make_async_copy(ins[i], out.at[0, rows, :], sems.at[i]))
        copies[-1].start()
    if header:
        head = refs[n + 1]
        top = stats[0][0:8, :]
        add = stats[0][8:24, :]
        for ref in stats[1:]:
            top = jnp.maximum(top, ref[0:8, :])
            add = add + ref[8:24, :]
        top = jnp.max(top, axis=1, keepdims=True)
        add = jnp.sum(add, axis=1, keepdims=True)
        count = add[0:4]
        divisor = jnp.maximum(count, 1.0)
        average = add[4:8] / divisor
        variance = add[8:12] / divisor - average * average
        columns = (-top[0:4], top[4:8], count / CELLS, average, jnp.sqrt(jnp.maximum(variance, 0.25)))
        for s, column in enumerate(columns):
            head[:, s : s + 1] = column
    for copy in copies:
        copy.wait()


def assemble(slots, ins, stats=None, half=None):
    header = stats is not None
    any_ = pl.BlockSpec(memory_space=pltpu.HBM)
    vmem = pl.BlockSpec(memory_space=pltpu.VMEM)
    n = len(slots)
    tile = jax.ShapeDtypeStruct((1, 256, WIDE), f32)
    return pl.pallas_call(
        functools.partial(assemble_kernel, slots, header),
        out_shape=[tile, jax.ShapeDtypeStruct((BANDS, 5), f32)] if header else tile,
        in_specs=([vmem] * 8 + [any_] if header else []) + [vmem] * n,
        out_specs=[any_, vmem] if header else any_,
        input_output_aliases={8: 0} if header else {},
        scratch_shapes=[pltpu.SemaphoreType.DMA((n,))],
        compiler_params=pltpu.CompilerParams(vmem_limit_bytes=12 << 20),
        cost_estimate=pl.CostEstimate(flops=1_000_000, bytes_accessed=n * 262144, transcendentals=0),
    )(*([*stats, half] if header else []), *ins)


def send(value, axes, size, keys):
    pairs = [(s, s ^ keys[s & 1]) for s in range(size)]
    return lax.ppermute(value, axes, pairs)


EARLY = 12


def on_device(pixels, flags):
    pixels = pltpu.with_memory_space_constraint(pixels, pltpu.HBM)
    flags = pltpu.with_memory_space_constraint(flags, pltpu.HBM)
    sent, acc = [], None
    for j, chunk in enumerate(CHUNKS):
        last = j == len(CHUNKS) - 1
        made, acc = pieces([SLOTS[i] for i in chunk], pixels, flags, acc, last)
        for i, piece in zip(chunk, made):
            sent.append(send(piece, GROUP, 16, SLOTS[i]) if SLOTS[i][0] else piece)
    s = acc
    s = merged(s, send(s, ("c",), 2, (1, 1)))
    s = merged(merged(s, send(s, ("x",), 4, (1, 1))), merged(send(s, ("x",), 4, (2, 2)), send(s, ("x",), 4, (3, 3))))
    s = merged(s, send(s, ("zh", "z"), 4, (3, 3)))
    stats = [s] + [send(s, ("z", "y"), 8, (k, k)) for k in range(1, 8)]
    order = list(range(15, 16)) + list(range(EARLY))
    half = assemble([SLOTS[i] for i in order], [sent[i] for i in order])
    order = list(range(EARLY, 15))
    tile, header = assemble([SLOTS[i] for i in order], [sent[i] for i in order], stats, half)
    return tile, header.T


def solution(mesh):
    split = Mesh(mesh.devices.reshape(4, 2, 2, 4, 2), ALL)
    placed = (P(None, ALL, None), P(None, ALL, None))
    return jax.shard_map(
        on_device, mesh=split, in_specs=placed, out_specs=(P(ALL, None, None), P()), check_vma=False
    )
```

```python
import functools

import jax
import jax.numpy as jnp
from jax import lax
from jax.experimental import pallas as pl
from jax.experimental.pallas import tpu as pltpu
from jax.sharding import Mesh
from jax.sharding import PartitionSpec as P


BANDS = 4
TILE = 512
STRIP = 16
WIDE = TILE * BANDS
CELLS = 16777216
BIG = 3e38
ALL = ("x", "zh", "z", "y", "c")
GROUP = ("z", "y", "c")
f32 = jnp.float32


Z, Y1, Y2, Y3, ZY1, ZY2, ZY3 = 8, 2, 4, 6, 10, 12, 14
SLOTS = [(ZY1, Y3), (Y1, ZY3), (ZY3, Y1), (Y3, ZY1), (Z, Y2), (Y2, Z), (ZY2, ZY2)]
OWN = (0, 0)
BLOCK = STRIP * WIDE // 1024
STAT = 3


def other(keys):
    return (keys[0] ^ 1, keys[1] ^ 1)


def crossed(keys):
    return (keys[1] ^ 1, keys[0] ^ 1)


FIRST = [[k, other(k)] for k in SLOTS[:2]]
SECOND = [[k, other(k)] for k in SLOTS[2:6]] + [[SLOTS[6]], [other(SLOTS[6])], [other(OWN)], [OWN]]


def position():
    z, y, c = (lax.axis_index(a) for a in GROUP)
    return z * 8 + y * 2 + c, c


def interleave(a, lane, pick):
    low = lane < 64
    even = (lane & 32) == 0
    u0 = jnp.where(low, a[0], pltpu.roll(a[2], 64, 1))
    u2 = jnp.where(low, pltpu.roll(a[0], 64, 1), a[2])
    u1 = jnp.where(low, a[1], pltpu.roll(a[3], 64, 1))
    u3 = jnp.where(low, pltpu.roll(a[1], 64, 1), a[3])
    v = [
        jnp.where(even, u0, pltpu.roll(u1, 32, 1)),
        jnp.where(even, pltpu.roll(u0, 96, 1), u1),
        jnp.where(even, u2, pltpu.roll(u3, 32, 1)),
        jnp.where(even, pltpu.roll(u2, 96, 1), u3),
    ]
    return [jnp.take_along_axis(t, pick, axis=1, mode="promise_in_bounds") for t in v]


def pieces_kernel(plan, last, px, fl, *refs):
    refs = list(refs)
    before = refs.pop(0) if last else None
    outs = refs[: len(plan)]
    stat, pbuf, fbuf, sems = refs[len(plan) :]
    pos, core = position()
    order = [(out, h, keys) for out, pieces in zip(outs, plan) for h, keys in enumerate(pieces)]
    copies = []
    for i, (_, _, (k0, k1)) in enumerate(order):
        cols = pl.ds(pl.multiple_of((pos ^ jnp.where(core == 0, k0, k1)) * TILE, TILE), TILE)
        pair = (
            pltpu.make_async_copy(px.at[:, :, cols], pbuf.at[i], sems.at[0, i]),
            pltpu.make_async_copy(fl.at[:, :, cols], fbuf.at[i], sems.at[1, i]),
        )
        for copy in pair:
            copy.start()
        copies.append(pair)
    lane = lax.broadcasted_iota(jnp.int32, (8, 128), 1)
    pick = 32 * (lane & 3) + (lane >> 2)
    if last:
        acc = [before[s] for s in range(20)]
    else:
        acc = [jnp.full((8, 128), -BIG, f32)] * 8 + [jnp.zeros((8, 128), f32)] * 12
    for i, (out, h, _) in enumerate(order):
        for copy in copies[i]:
            copy.wait()
        for r in range(STRIP // 8):
            for s in range(TILE // 128):
                part = []
                for b in range(BANDS):
                    v = pbuf[i, b, r * 8 : r * 8 + 8, s * 128 : s * 128 + 128]
                    use = fbuf[i, b, r * 8 : r * 8 + 8, s * 128 : s * 128 + 128] == 1
                    m = jnp.where(use, v, 0.0)
                    acc[b] = jnp.maximum(acc[b], jnp.where(use, -v, -BIG))
                    acc[4 + b] = jnp.maximum(acc[4 + b], jnp.where(use, v, -BIG))
                    acc[8 + b] += jnp.where(use, 1.0, 0.0)
                    acc[12 + b] += m
                    acc[16 + b] += m * m
                    part.append(m)
                for j, o in enumerate(interleave(part, lane, pick)):
                    out[h * BLOCK + r * 16 + s * 4 + j] = o
    if not last:
        for s in range(20):
            stat[s] = acc[s]
        return
    zero = jnp.zeros((1, 128), f32)
    lines = [(jnp.max if s < 8 else jnp.sum)(a, axis=0, keepdims=True) for s, a in enumerate(acc)] + [zero] * 4
    for t in range(STAT):
        stat[t] = jnp.concatenate(lines[8 * t : 8 * t + 8], axis=0)


def pieces(plan, pixels, flags, before=None):
    hbm = pl.BlockSpec(memory_space=pltpu.HBM)
    vmem = pl.BlockSpec(memory_space=pltpu.VMEM)
    last = before is not None
    count = [len(keys) * BLOCK for keys in plan] + [STAT if last else 20]
    n = sum(len(keys) for keys in plan)
    return pl.pallas_call(
        functools.partial(pieces_kernel, plan, last),
        out_shape=[jax.ShapeDtypeStruct((c, 8, 128), f32) for c in count],
        in_specs=[hbm, hbm] + [vmem] * last,
        out_specs=[vmem] * len(count),
        scratch_shapes=[
            pltpu.VMEM((n, BANDS, STRIP, TILE), f32),
            pltpu.VMEM((n, BANDS, STRIP, TILE), jnp.int32),
            pltpu.SemaphoreType.DMA((2, n)),
        ],
        compiler_params=pltpu.CompilerParams(vmem_limit_bytes=12 << 20),
        cost_estimate=pl.CostEstimate(flops=n * 250_000, bytes_accessed=n * 393216, transcendentals=0),
    )(pixels, flags, *([before] if last else []))


def merged(a, b):
    tile = lax.broadcasted_iota(jnp.int32, (STAT, 8, 128), 0)
    return jnp.where(tile == 0, jnp.maximum(a, b), a + b)


def assemble_kernel(places, stats, half, *refs):
    refs = list(refs)
    stat = refs[:stats]
    ins = refs[stats + half : stats + half + len(places)]
    out, sems = refs[stats + half + len(places)], refs[-1]
    pos, core = position()
    copies = []
    for source, sources in zip(ins, places):
        for at, keys in enumerate(sources):
            if keys is None:
                continue
            rows = pl.ds(pl.multiple_of((pos ^ jnp.where(core == 0, *keys)) * BLOCK, BLOCK), BLOCK)
            part = source.at[at * BLOCK : (at + 1) * BLOCK]
            copies.append(pltpu.make_async_copy(part, out.at[rows], sems.at[len(copies)]))
            copies[-1].start()
    if stats:
        head = refs[-2]
        top = stat[0][0]
        add = [stat[0][1], stat[0][2]]
        for ref in stat[1:]:
            top = jnp.maximum(top, ref[0])
            add = [add[0] + ref[1], add[1] + ref[2]]
        top = jnp.max(top, axis=1, keepdims=True)
        add = [jnp.sum(a, axis=1, keepdims=True) for a in add]
        count = add[0][0:4]
        divisor = jnp.maximum(count, 1.0)
        average = add[0][4:8] / divisor
        variance = add[1][0:4] / divisor - average * average
        columns = (-top[0:4], top[4:8], count / CELLS, average, jnp.sqrt(jnp.maximum(variance, 0.25)))
        for s, column in enumerate(columns):
            head[:, s : s + 1] = column
    for copy in copies:
        copy.wait()


def assemble(pairs, half=None, stats=()):
    ins, places = [p[0] for p in pairs], [p[1] for p in pairs]
    hbm = pl.BlockSpec(memory_space=pltpu.HBM)
    vmem = pl.BlockSpec(memory_space=pltpu.VMEM)
    tile = jax.ShapeDtypeStruct((16 * BLOCK, 8, 128), f32)
    halves = [] if half is None else [half]
    return pl.pallas_call(
        functools.partial(assemble_kernel, places, len(stats), len(halves)),
        out_shape=[tile, jax.ShapeDtypeStruct((BANDS, 5), f32)] if stats else tile,
        in_specs=[vmem] * len(stats) + [hbm] * len(halves) + [vmem] * len(ins),
        out_specs=[hbm, vmem] if stats else hbm,
        input_output_aliases={len(stats): 0} if halves else {},
        scratch_shapes=[pltpu.SemaphoreType.DMA((16,))],
        compiler_params=pltpu.CompilerParams(vmem_limit_bytes=12 << 20),
        cost_estimate=pl.CostEstimate(flops=1_000_000, bytes_accessed=1 << 20, transcendentals=0),
    )(*stats, *halves, *ins)


def send(value, axes, size, keys):
    pairs = [(s, s ^ keys[s & 1]) for s in range(size)]
    return lax.ppermute(value, axes, pairs)


ROUNDS = [(("c",), 2, 1), (("x",), 4, 1), (("x",), 4, 3), (("zh", "z"), 4, 3)]
ASK = [(Z, Y1), (Y3, Y2), (ZY1, ZY3), (ZY2, ZY2)]


def on_device(pixels, flags):
    pixels = pltpu.with_memory_space_constraint(pixels, pltpu.HBM)
    flags = pltpu.with_memory_space_constraint(flags, pltpu.HBM)
    *made, stat = pieces(FIRST, pixels, flags)
    *more, theirs, mine, stat = pieces(SECOND, pixels, flags, stat)
    keys = SLOTS + [other(SLOTS[6])]
    got = [send(v, GROUP, 16, keys[i]) for i, v in enumerate(made + more)]
    swap = send(theirs, ("c",), 2, (1, 1))
    passed = []
    for j in (0, 3):
        halves = jnp.concatenate([got[i][BLOCK : 2 * BLOCK] for i in range(j, j + 3)], axis=0)
        passed.append(send(halves, ("c",), 2, (1, 1)))
    for axes, size, key in ROUNDS:
        stat = merged(stat, send(stat, axes, size, (key, key)))
    heard = [send(stat, GROUP, 16, k) for k in ASK]
    told = functools.reduce(merged, heard[:3])
    rest = send(told, ("c",), 2, (1, 1))
    landed = [(got[i], [SLOTS[i]]) for i in range(6)]
    relayed = [(v, [crossed(SLOTS[i]) for i in range(j, j + 3)]) for v, j in zip(passed, (0, 3))]
    ends = [(got[6], [keys[6]]), (got[7], [keys[7]])]
    half = assemble([(mine, [OWN]), (swap, [other(OWN)])] + landed[:3] + relayed[:1])
    tile, header = assemble(landed[3:] + relayed[1:] + ends, half, [stat, told, rest, heard[3]])
    tile = tile.reshape(1, 32, 16, 8, 128).transpose(0, 1, 3, 2, 4).reshape(1, 256, WIDE)
    return tile, header.T


def solution(mesh):
    split = Mesh(mesh.devices.reshape(4, 2, 2, 4, 2), ALL)
    placed = (P(None, ALL, None), P(None, ALL, None))
    return jax.shard_map(
        on_device, mesh=split, in_specs=placed, out_specs=(P(ALL, None, None), P()), check_vma=False
    )
```
